32 devices in a mesh: tensor: 8 (over z, y), dp: 4 (over x, core).
Axes of the slice: x: 2, y: 2, z: 4, core: 2. Of those that a mesh axis runs over, the one named last changes fastest.
Arguments:
- base_weight: bfloat16 [2, 2, 4096, 14336], P(None, None, 'tensor', 'dp'), may hold values from -0.125 to 0.125
- adapter_left: bfloat16 [2, 2, 4096, 16], P(None, None, 'tensor'), may hold values from -0.059814453 to 0.059814453
- adapter_right: bfloat16 [2, 2, 16, 14336], P(None, None, None, 'dp'), may hold values from -1.5 to 1.5
- magnitude: bfloat16 [2, 2, 14336], P(None, None, 'dp'), may hold values from 16 to 256
Outputs:
- merged_weight: bfloat16 [2, 2, 14336, 4096], P(None, None, 'tensor')
The draws below stay inside these ranges and needn't reach their ends.
All inputs are finite; a program needn't handle non-finite values.
Results may differ from the reference program's by a relative error of at most 0.0004.
Values may be sent and summed in bfloat16 or wider, within the bound.
A program may use at most 384 MiB of HBM per device.

```python
import math
import jax
import jax.numpy as jnp
from jax import lax

D = 4096
FF = 14336
RANK = 16
EXP = 2
PROJ = 2


def with_spikes(result, key, source, target, blocks, factor):
    def block_of(axis_at):
        return (jnp.arange(result.shape[axis_at]) // (result.shape[axis_at] // blocks)).reshape((-1,) + (1,) * (result.ndim - 1 - axis_at))

    first = jax.random.permutation(key, blocks)[block_of(target)]
    second = (block_of(target) + blocks // 2) % blocks
    return jnp.where((block_of(source) == first) | (block_of(source) == second), factor * result, result)


def block_scale(key, shape, pieces, low, high):
    def one(dim, parts):
        heights = jax.random.uniform(jax.random.fold_in(jax.random.fold_in(key, 6), dim), (parts,), jnp.float32, low / len(pieces), high / len(pieces))
        return jnp.repeat(jnp.exp(heights), shape[dim] // parts).reshape((-1,) + (1,) * (len(shape) - dim - 1))

    level = one(*pieces[0])
    for cut in pieces[1:]:
        level = level * one(*cut)
    return level


def noise(rng, extent, scale, bound, cuts=(), dtype=jnp.bfloat16):
    entries = scale * jax.random.normal(rng, extent, jnp.float32)
    if cuts:
        entries = entries * block_scale(rng, extent, cuts, -0.22, 0.18)
    return jnp.clip(entries, -bound, bound).astype(dtype)


def bell_draw_with(stream_key, extent, deviation, most, pieces, heavy, kind=jnp.bfloat16):
    drawn = deviation * jax.random.normal(stream_key, extent, jnp.float32)
    if pieces:
        drawn = drawn * block_scale(stream_key, extent, pieces, -0.22, 0.18)
    return jnp.clip(with_spikes(drawn, jax.random.fold_in(stream_key, 3), *heavy), -most, most).astype(kind)


def setup_inputs(seed: int = 0) -> dict:
    key_of = jax.random.split(jax.random.key(seed), 5)
    return {
        "base_weight": bell_draw_with(key_of[0], (EXP, PROJ, D, FF), D ** -0.5, 0.125, ((2, 8), (3, 4)), (2, 3, 8, 2.0)),
        "adapter_left": noise(key_of[1], (EXP, PROJ, D, RANK), 0.01, 0.059814453, ((2, 8),)),
        "adapter_right": noise(key_of[2], (EXP, PROJ, RANK, FF), RANK ** -0.5, 1.5, ((3, 4),)),
        "magnitude": jnp.clip(jnp.exp(math.log(256.0) - 2.7725887 * jax.random.uniform(key_of[3], (EXP, PROJ, FF), jnp.float32) ** block_scale(key_of[3], (EXP, PROJ, FF), ((2, 4),), -0.2, 0.2)), 16.0, 256.0).astype(jnp.bfloat16),
    }


def merge_one(operands):
    weight, left_factor, right_factor, column_scale = operands
    merged = weight.astype(jnp.float32) + jnp.dot(left_factor, right_factor, preferred_element_type=jnp.float32)
    squares = lax.optimization_barrier(jnp.sum(merged * merged, axis=0))
    scaling = column_scale.astype(jnp.float32) / jnp.sqrt(squares + 1e-06)
    return (merged * scaling[None, :]).astype(jnp.bfloat16).T

def reference(base_weight, adapter_left, adapter_right, magnitude):
    stacked = lax.map(merge_one, (base_weight.reshape(EXP * PROJ, D, FF), adapter_left.reshape(EXP * PROJ, D, RANK), adapter_right.reshape(EXP * PROJ, RANK, FF), magnitude.reshape(EXP * PROJ, FF)))
    return stacked.reshape(EXP, PROJ, FF, D)
```

```python
import functools

import jax
import jax.numpy as jnp
from jax import lax
from jax.experimental import pallas as pl
from jax.experimental.pallas import tpu as pltpu
from jax.sharding import PartitionSpec as P

MESH = pl.DeviceIdType.MESH


def exchange_kernel(sizes, chunks, relayed, s, g, rb, recv, xs, cs, a_send, a_recv, b_send, r_send):
    tensor_count, replica_count = sizes
    group = tensor_count // replica_count
    half_t, half_r = tensor_count // 2, replica_count // 2
    serve = s.shape[3]
    parts = ((0, relayed), (relayed, serve - relayed))
    t, d = lax.axis_index("tensor"), lax.axis_index("dp")
    twin = lax.rem(d + half_r, replica_count)
    mate = d + 1 - 2 * lax.rem(d, 2)
    near = t // half_t == d // half_r
    far = jnp.logical_not(near)
    home = t // group
    is_home, is_twin = home == d, home == twin
    base = (t // half_t) * half_t
    other = half_t - base

    def near_source(i):
        return base + lax.rem(t - base + i, half_t)

    def far_source(i):
        return other + lax.rem(t - base + i, half_t)

    def own(k, j, p):
        return s.at[k, j, :, pl.ds(*parts[p])]

    def slot(ts, k, p):
        return g.at[ts, k, :, pl.ds(*parts[p])]

    def send(src, ts, k, p, sem, tensor, dp):
        return pltpu.make_async_remote_copy(
            src_ref=src, dst_ref=slot(ts, k, p), send_sem=sem, recv_sem=recv.at[ts, k, p],
            device_id={"tensor": tensor, "dp": dp}, device_id_type=MESH,
        )

    def to_twin(src, ts, k, p):
        return send(src, ts, k, p, xs.at[ts, k, p], t, twin)

    def to_mate(src, ts, k, p):
        return send(src, ts, k, p, cs.at[ts, k, p], t, mate)

    def to_relay(k, j):
        return pltpu.make_async_remote_copy(
            src_ref=own(k, j, 0), dst_ref=rb.at[k, j], send_sem=a_send.at[k, j], recv_sem=a_recv.at[k, j],
            device_id={"tensor": t, "dp": twin}, device_id_type=MESH,
        )

    def relay(k, j):
        return send(rb.at[k, j], t, k, 0, r_send.at[k, j], twin * group + j, d)

    def direct(k, j, p):
        return send(own(k, j, p), t, k, p, b_send.at[k, j, p], d * group + j, d)

    def keep(k, p):
        return pltpu.make_async_copy(own(k, lax.rem(t, group), p), slot(t, k, p), recv.at[t, k, p])

    def got(ts, k, p):
        to_mate(slot(ts, k, p), ts, k, p).wait_recv()

    def loop(count, body, first=0):
        lax.fori_loop(first, count, lambda i, c: (body(i), c)[1], 0)

    def each_piece(body):
        loop(chunks, lambda k: loop(group, lambda j: body(k, j)))

    def start_piece(k, j):
        leaves = d * group + j != t

        @pl.when(far)
        def _():
            to_relay(k, j).start()
            direct(k, j, 1).start()

        @pl.when(jnp.logical_and(near, leaves))
        def _():
            direct(k, j, 0).start()
            direct(k, j, 1).start()

        @pl.when(jnp.logical_not(leaves))
        def _():
            for p in range(2):
                src = own(k, j, p)
                to_twin(src, t, k, p).start()
                to_mate(src, t, k, p).start()
                keep(k, p).start()

    each_piece(start_piece)

    def pass_on(ts, k, p):
        got(ts, k, p)
        to_twin(slot(ts, k, p), ts, k, p).start()
        to_mate(slot(ts, k, p), ts, k, p).start()

    def hand_over(ts, k, p):
        got(ts, k, p)
        to_mate(slot(ts, k, p), ts, k, p).start()

    def relay_step(k):
        @pl.when(near)
        def _():
            def one(j):
                to_relay(k, j).wait_recv()
                relay(k, j).start()

            loop(group, one)

    def arrivals(k):
        @pl.when(is_home)
        def _():
            def one(i):
                pass_on(near_source(i), k, 0)
                pass_on(near_source(i), k, 1)

            loop(half_t, one, 1)
            loop(half_t, lambda i: pass_on(far_source(i), k, 1))

        @pl.when(is_twin)
        def _():
            loop(half_t, lambda i: pass_on(far_source(i), k, 0))

    def second_hand(k):
        @pl.when(is_home)
        def _():
            loop(half_t, lambda i: hand_over(far_source(i), k, 0))

        @pl.when(is_twin)
        def _():
            def one(i):
                hand_over(near_source(i), k, 0)
                hand_over(near_source(i), k, 1)

            loop(half_t, one)
            loop(half_t, lambda i: hand_over(far_source(i), k, 1))

    relay_step(0)

    def step(k):
        @pl.when(k + 1 < chunks)
        def _():
            relay_step(k + 1)

        arrivals(k)

        @pl.when(k > 0)
        def _():
            second_hand(k - 1)

    loop(chunks, step)
    second_hand(chunks - 1)

    serving = jnp.logical_or(is_home, is_twin)

    @pl.when(jnp.logical_not(serving))
    def _():
        def one(k, ts):
            got(ts, k, 0)
            got(ts, k, 1)

        loop(chunks, lambda k: loop(tensor_count, lambda ts: one(k, ts)))

    @pl.when(is_home)
    def _():
        def one(k):
            keep(k, 0).wait()
            keep(k, 1).wait()

        loop(chunks, one)

    def finish_piece(k, j):
        leaves = d * group + j != t

        @pl.when(far)
        def _():
            to_relay(k, j).wait_send()
            direct(k, j, 1).wait_send()

        @pl.when(near)
        def _():
            relay(k, j).wait_send()

        @pl.when(jnp.logical_and(near, leaves))
        def _():
            direct(k, j, 0).wait_send()
            direct(k, j, 1).wait_send()

    each_piece(finish_piece)

    @pl.when(serving)
    def _():
        def one(k, ts):
            to_mate(slot(ts, k, 0), ts, k, 0).wait_send()
            to_mate(slot(ts, k, 1), ts, k, 1).wait_send()

        loop(chunks, lambda k: loop(tensor_count, lambda ts: one(k, ts)))

    @pl.when(is_home)
    def _():
        def one(k, i):
            to_twin(slot(near_source(i), k, 0), near_source(i), k, 0).wait_send()
            to_twin(slot(near_source(i), k, 1), near_source(i), k, 1).wait_send()
            to_twin(slot(far_source(i), k, 1), far_source(i), k, 1).wait_send()

        loop(chunks, lambda k: loop(half_t, lambda i: one(k, i)))

    @pl.when(is_twin)
    def _():
        def one(k, i):
            to_twin(slot(far_source(i), k, 0), far_source(i), k, 0).wait_send()

        loop(chunks, lambda k: loop(half_t, lambda i: one(k, i)))


def exchange(s, tensor_count, replica_count, relayed):
    chunks, group, each, serve, rows = s.shape
    dma = pltpu.SemaphoreType.DMA
    g, _ = pl.pallas_call(
        functools.partial(exchange_kernel, (tensor_count, replica_count), chunks, relayed),
        out_shape=(
            jax.ShapeDtypeStruct((tensor_count, chunks, each, serve, rows), s.dtype),
            jax.ShapeDtypeStruct((chunks, group, each, relayed, rows), s.dtype),
        ),
        in_specs=[pl.BlockSpec(memory_space=pl.ANY)],
        out_specs=[pl.BlockSpec(memory_space=pl.ANY)] * 2,
        scratch_shapes=[dma((tensor_count, chunks, 2))] * 3
        + [dma((chunks, group))] * 2
        + [dma((chunks, group, 2)), dma((chunks, group))],
        compiler_params=pltpu.CompilerParams(has_side_effects=True),
    )(s)
    return g


def flip_kernel(w, o):
    o[0] = w[0].T


def flip(w):
    stacks, rows, cols = w.shape
    if rows % 128:
        return w.swapaxes(1, 2)
    wide = next(n for n in (512, 256, 128, cols) if cols % n == 0)
    return pl.pallas_call(
        flip_kernel,
        grid=(stacks, cols // wide),
        in_specs=[pl.BlockSpec((1, rows, wide), lambda e, c: (e, 0, c))],
        out_specs=pl.BlockSpec((1, wide, rows), lambda e, c: (e, c, 0)),
        out_shape=jax.ShapeDtypeStruct((stacks, cols, rows), w.dtype),
    )(w)


def merge_kernel(count, rows, g, left, right, magnitude, o, merged):
    squares = None
    for n in range(count):
        at = slice(n * rows, (n + 1) * rows)
        piece = g[n, 0].astype(jnp.float32) + jnp.dot(
            right[0], left[0, :, at], preferred_element_type=jnp.float32
        )
        merged[:, at] = piece
        total = jnp.sum(piece * piece, axis=1, keepdims=True)
        squares = total if squares is None else squares + total
    scaling = magnitude[0].astype(jnp.float32) / jnp.sqrt(squares + 1e-06)
    for n in range(count):
        at = slice(n * rows, (n + 1) * rows)
        o[0, :, at] = (merged[:, at] * scaling).astype(o.dtype)


def merge(g, left, right, magnitude):
    count, stacks, serve, rows = g.shape
    rank = right.shape[2]
    if rows % 128:
        joined = g.transpose(1, 2, 0, 3).reshape(stacks, serve, count * rows)
        merged = joined.astype(jnp.float32) + jnp.einsum(
            "xfr,xri->xfi", right, left, preferred_element_type=jnp.float32
        )
        squares = jnp.sum(merged * merged, axis=2, keepdims=True)
        scaling = magnitude.astype(jnp.float32) / jnp.sqrt(squares + 1e-06)
        return (merged * scaling).astype(g.dtype)
    tall = next(n for n in (256, 128, 64, 32, 16, serve) if serve % n == 0)
    return pl.pallas_call(
        functools.partial(merge_kernel, count, rows),
        grid=(stacks, serve // tall),
        in_specs=[
            pl.BlockSpec((count, 1, tall, rows), lambda e, f: (0, e, f, 0)),
            pl.BlockSpec((1, rank, count * rows), lambda e, f: (e, 0, 0)),
            pl.BlockSpec((1, tall, rank), lambda e, f: (e, f, 0)),
            pl.BlockSpec((1, tall, 1), lambda e, f: (e, f, 0)),
        ],
        out_specs=pl.BlockSpec((1, tall, count * rows), lambda e, f: (e, f, 0)),
        out_shape=jax.ShapeDtypeStruct((stacks, serve, count * rows), g.dtype),
        scratch_shapes=[pltpu.VMEM((tall, count * rows), jnp.float32)],
    )(g, left, right, magnitude)


def shards(base_weight, adapter_left, adapter_right, magnitude):
    tensor_count = lax.axis_size("tensor")
    replica_count = lax.axis_size("dp")
    experts, projections, rows, cols = base_weight.shape
    rank = adapter_left.shape[3]
    stacks = experts * projections
    group = tensor_count // replica_count
    serve = cols // group
    chunks = stacks if tensor_count <= 16 else 1
    relayed = (2 * (serve // 16) + 1) // 3 * 16

    s = flip(base_weight.reshape(stacks, rows, cols))
    if chunks == 1:
        s = s.reshape(1, stacks, group, serve, rows).swapaxes(1, 2)
    else:
        s = s.reshape(chunks, group, 1, serve, rows)
    g = exchange(s, tensor_count, replica_count, relayed).reshape(tensor_count, stacks, serve, rows)

    left = lax.all_gather(adapter_left.swapaxes(2, 3), "tensor", axis=3, tiled=True)
    right_all = lax.all_gather(adapter_right, "dp", axis=3, tiled=True)
    magnitude_all = lax.all_gather(magnitude, "dp", axis=2, tiled=True)
    start = lax.axis_index("tensor") * serve
    right = lax.dynamic_slice_in_dim(right_all, start, serve, 3).swapaxes(2, 3)
    strength = lax.dynamic_slice_in_dim(magnitude_all, start, serve, 2)
    out = merge(
        g,
        left.reshape(stacks, rank, -1),
        right.reshape(stacks, serve, rank),
        strength.reshape(stacks, serve, 1),
    )
    return out.reshape(experts, projections, serve, -1)


def solution(mesh):
    in_specs = (
        P(None, None, "tensor", "dp"),
        P(None, None, "tensor", None),
        P(None, None, None, "dp"),
        P(None, None, "dp"),
    )
    out_specs = P(None, None, "tensor", None)
    return jax.shard_map(shards, mesh=mesh, in_specs=in_specs, out_specs=out_specs, check_vma=False)
```
